64 devices in a mesh: dp: 4 (over x, y), vp: 16 (over z, core).
Axes of the slice: x: 2, y: 2, z: 8, core: 2. Of those that a mesh axis runs over, the one named last changes fastest.
The devices are a block of a 4x4x8 slice.
Arguments:
- hidden: bfloat16 [4096, 8192], P('dp'), parts along dimension 0
- w_head: bfloat16 [8192, 32000], P(None, 'vp')
- inv_temp: float32 [4096], P('dp'), parts along dimension 0
- target: int32 [4096], P('dp'), parts along dimension 0
Outputs:
- output 1: float32 [4096, 32000], P('dp', 'vp'), parts along dimension 0
- output 2: float32 [4096], P('dp'), parts along dimension 0
There are 4 independent parts. The reference program is written for one: setup_inputs(seed, part) draws one part's arguments, and reference() takes and returns one part's arrays. A program takes and returns all parts, laid end to end along the dimension named above; an argument that names none is the same for every part.
All inputs are finite; a program needn't handle non-finite values.
Results may differ from the reference program's by a relative error of at most 0.001.
Values are sent between devices in bfloat16 or wider.
A program may use at most 768 MiB of HBM per device.

```python
import math
import jax
import jax.numpy as jnp

ROWS = 1024
D = 8192
V = 32000


def setup_inputs(seed: int = 0, part: int = 0) -> dict:
    shared_key = jax.random.key(seed)
    key_wnoise, key_wlead = jax.random.split(shared_key)
    part_key = jax.random.fold_in(jax.random.key(seed + 1), part)
    key_hidden, key_lead, key_temp, key_target = jax.random.split(part_key, 4)
    lead_dims = 4
    ramp = 1.0 - 2.0 * jnp.arange(V, dtype=jnp.float32) / (V - 1)
    w_lead = 0.5 * ramp[None, :] * (1.0 + 0.25 * jax.random.normal(key_wlead, (lead_dims, V), jnp.float32))
    w_rest = jax.random.normal(key_wnoise, (D - lead_dims, V), jnp.float32) * (D ** -0.5)
    w_head = jnp.concatenate([w_lead, w_rest], axis=0).astype(jnp.bfloat16)
    h_lead = 1.0 + 0.3 * jax.random.normal(key_lead, (ROWS, lead_dims), jnp.float32)
    h_rest = jax.random.normal(key_hidden, (ROWS, D - lead_dims), jnp.float32)
    hidden = jnp.concatenate([h_lead, h_rest], axis=1).astype(jnp.bfloat16)
    inv_temp = jnp.exp(jax.random.uniform(key_temp, (ROWS,), jnp.float32, math.log(0.5), math.log(16.0)))
    low_id = V // 4
    target = jax.random.randint(key_target, (ROWS,), low_id, V, jnp.int32)
    target = target.at[0].set(low_id).at[1].set(V - 1)
    return {"hidden": hidden, "w_head": w_head, "inv_temp": inv_temp, "target": target}


def reference(hidden, w_head, inv_temp, target):
    logits = jnp.dot(hidden, w_head, preferred_element_type=jnp.float32) * inv_temp[:, None]
    row_max = jnp.max(logits, axis=1, keepdims=True)
    exp_vals = jnp.exp(logits - row_max)
    row_total = jnp.sum(exp_vals, axis=1, keepdims=True)
    cdf_table = jnp.cumsum(exp_vals / row_total, axis=1)
    cdf_target = jnp.take_along_axis(cdf_table, target[:, None], axis=1)[:, 0]
    return cdf_table, cdf_target
```

```python
import functools

import jax
import jax.numpy as jnp
from jax import lax
from jax.experimental import pallas as pl
from jax.experimental.pallas import tpu as pltpu
from jax.sharding import PartitionSpec as P

LANES = 128
SUB = 8
TILE = 400
FOLD = 10
UNIT = 512
DEPTH = 1024
AHEAD = 2
F32 = jnp.float32
NT = (((1,), (1,)), ((), ()))


def head_kernel(n_dev, h_hbm, w_hbm, tau_ref, tgt_ref, sums_ref, gain_ref, off_ref, tsum_ref,
                w_ref, ha_ref, hb_ref, stat_ref, snd, rcv,
                w_sem, ha_sem, hb_sem, send_sem, recv_sem):
    width, depth = w_hbm.shape
    n_k = depth // DEPTH
    per_unit = UNIT // LANES
    n_tile = width // TILE
    me = lax.axis_index("vp")

    barrier = pltpu.get_barrier_semaphore()

    @pl.loop(1, n_dev)
    def _(d):
        pl.semaphore_signal(barrier, inc=1, device_id={"vp": lax.rem(me + d, n_dev)},
                            device_id_type=pl.DeviceIdType.MESH)

    def w_copy(k):
        ks = pl.ds(pl.multiple_of(k * DEPTH, DEPTH), DEPTH)
        return pltpu.make_async_copy(w_hbm.at[:, ks], w_ref.at[:, ks], w_sem.at[k])

    def ha_copy(k):
        slot = lax.rem(k, AHEAD)
        ks = pl.ds(pl.multiple_of(k * DEPTH, DEPTH), DEPTH)
        return pltpu.make_async_copy(h_hbm.at[pl.ds(0, UNIT), ks], ha_ref.at[slot], ha_sem.at[slot])

    def hb_copy():
        return pltpu.make_async_copy(h_hbm.at[pl.ds(UNIT, UNIT), :], hb_ref, hb_sem.at[0])

    for k in range(AHEAD):
        w_copy(k).start()
        ha_copy(k).start()

    sums_ref[0:per_unit] = jnp.zeros((per_unit, width, LANES), F32)
    first = me * width
    shape = (TILE // SUB, SUB, LANES)
    sub = lax.broadcasted_iota(jnp.int32, shape, 1)
    token = lax.broadcasted_iota(jnp.int32, shape, 0) * SUB + sub

    def finish(g, t, z):
        n = TILE // SUB
        z = (z * tau_ref[g:g + 1, :]).reshape(shape)
        top = jnp.max(jnp.max(z, axis=0), axis=0, keepdims=True)
        p = jnp.exp(z - top[None])
        local = tgt_ref[g:g + 1, :] - (first + t * TILE)
        upto = jnp.sum(jnp.where(token <= local[None], p, 0.0), axis=0)
        stat_ref[g, t:t + 1, :] = top
        stat_ref[g, 2 * n_tile + t:2 * n_tile + t + 1, :] = jnp.sum(upto, axis=0, keepdims=True)
        for s in (1, 2, 4):
            p = p + jnp.where(sub >= s, pltpu.roll(p, s, 1), 0.0)
        last = jnp.broadcast_to(p[:, SUB - 1:, :], shape).reshape(n // FOLD, FOLD, SUB, LANES)
        p = p.reshape(n // FOLD, FOLD, SUB, LANES)
        run = last[:, 0]
        cols = [p[:, 0]]
        for i in range(1, FOLD):
            cols.append(p[:, i] + run)
            run = run + last[:, i]
        ahead = jnp.zeros((1, SUB, LANES), F32)
        starts = []
        for i in range(n // FOLD):
            starts.append(ahead)
            ahead = ahead + run[i:i + 1]
        p = jnp.stack(cols, axis=1) + jnp.concatenate(starts, axis=0)[:, None]
        sums_ref[g, t * TILE:(t + 1) * TILE, :] = p.reshape(TILE, LANES)
        stat_ref[g, n_tile + t:n_tile + t + 1, :] = ahead[0, 0:1, :]

    def finish_step(u, t, z):
        for j in range(per_unit):
            finish(u * per_unit + j, t, z[:, j * LANES:(j + 1) * LANES])

    def peer_copy(u, d):
        peer = lax.rem(me + d, n_dev)
        return pltpu.make_async_remote_copy(
            src_ref=snd.at[u], dst_ref=rcv.at[u, me], send_sem=send_sem.at[u, peer],
            recv_sem=recv_sem.at[u, me], device_id={"vp": peer}, device_id_type=pl.DeviceIdType.MESH)

    def send_unit(u):
        for j in range(per_unit):
            g = u * per_unit + j
            top_t = stat_ref[g, 0:n_tile, :]
            top = jnp.max(top_t, axis=0, keepdims=True)
            e = jnp.exp(top_t - top)
            s = jnp.sum(e * stat_ref[g, n_tile:2 * n_tile, :], axis=0, keepdims=True)
            t = jnp.sum(e * stat_ref[g, 2 * n_tile:3 * n_tile, :], axis=0, keepdims=True)
            for i, x in enumerate((top, s, t)):
                snd[u, i, j:j + 1, :] = x
                rcv[u, me, i, j:j + 1, :] = x

        @pl.loop(1, n_dev)
        def _(d):
            peer_copy(u, d).start()

    def receive_unit(u):
        @pl.loop(1, n_dev)
        def _(d):
            src = lax.rem(me + d, n_dev)
            pltpu.make_async_remote_copy(
                src_ref=snd.at[u], dst_ref=rcv.at[u, src], send_sem=send_sem.at[u, src],
                recv_sem=recv_sem.at[u, src], device_id={"vp": src},
                device_id_type=pl.DeviceIdType.MESH).wait()

        tops = rcv[u, :, 0]
        peak = jnp.max(tops, axis=0)
        e = jnp.exp(tops - peak[None])
        part = rcv[u, :, 1] * e
        total = jnp.sum(part, axis=0)
        device = lax.broadcasted_iota(jnp.int32, part.shape, 0)
        before = jnp.sum(jnp.where(device < me, part, 0.0), axis=0)
        upto = jnp.sum(rcv[u, :, 2] * e, axis=0)
        inv = 1.0 / total
        tsum_ref[u * per_unit:(u + 1) * per_unit, :] = upto * inv
        for j in range(per_unit):
            g = u * per_unit + j
            a_t = jnp.exp(stat_ref[g, 0:n_tile, :] - peak[j:j + 1, :])
            s_t = stat_ref[g, n_tile:2 * n_tile, :] * a_t
            gain_ref[g] = a_t * inv[j:j + 1, :]
            run = before[j:j + 1, :]
            for t in range(n_tile):
                off_ref[g, t:t + 1, :] = run * inv[j:j + 1, :]
                run = run + s_t[t:t + 1, :]

    def first_rows(k, last):
        w_copy(k).wait()
        ha_copy(k).wait()
        slot = lax.rem(k, AHEAD)
        ks = pl.ds(pl.multiple_of(k * DEPTH, DEPTH), DEPTH)
        for t in range(n_tile):
            ts = slice(t * TILE, (t + 1) * TILE)
            z = lax.dot_general(w_ref[ts, ks], ha_ref[slot], NT, preferred_element_type=F32)
            for j in range(per_unit):
                part = sums_ref[j, ts, :] + z[:, j * LANES:(j + 1) * LANES]
                if last:
                    finish(j, t, part)
                else:
                    sums_ref[j, ts, :] = part

    @pl.loop(0, n_k - 1)
    def _(k):
        first_rows(k, False)

        @pl.when(k + AHEAD < n_k)
        def _():
            w_copy(k + AHEAD).start()
            ha_copy(k + AHEAD).start()

        @pl.when(k + AHEAD == n_k)
        def _():
            hb_copy().start()

    first_rows(n_k - 1, True)
    pl.semaphore_wait(barrier, n_dev - 1)
    send_unit(0)

    hb_copy().wait()
    for t in range(n_tile):
        z = lax.dot_general(w_ref[t * TILE:(t + 1) * TILE, :], hb_ref[...], NT, preferred_element_type=F32)
        finish_step(1, t, z)
    send_unit(1)

    for u in range(2):
        receive_unit(u)


def write_kernel(sums_ref, gain_ref, off_ref, tsum_ref, out_hbm, tgt_out, stage, sem):
    groups, width, _ = sums_ref.shape
    slots, chunk = stage.shape[0], stage.shape[1]
    tgt_out[...] = tsum_ref[...]
    n = width // chunk

    def out_copy(i):
        return pltpu.make_async_copy(stage.at[i % slots], out_hbm.at[pl.ds(i * chunk, chunk), :], sem.at[i % slots])

    for i in range(n):
        if i >= slots:
            out_copy(i - slots).wait()
        rs = slice(i * chunk, (i + 1) * chunk)
        t = i * chunk // TILE
        for g in range(groups):
            stage[i % slots, :, g * LANES:(g + 1) * LANES] = (
                sums_ref[g, rs, :] * gain_ref[g, t:t + 1, :] + off_ref[g, t:t + 1, :])
        out_copy(i).start()
    for i in range(max(0, n - slots), n):
        out_copy(i).wait()


def solution(mesh):
    n_dev = mesh.shape["vp"]

    def local_fn(h_rows, w_cols, tau_rows, tgt_rows):
        rows, depth = h_rows.shape
        width = w_cols.shape[1]
        groups = rows // LANES
        n_unit = rows // UNIT
        n_k = depth // DEPTH
        n_tile = width // TILE
        per_unit = UNIT // LANES
        vmem = pl.BlockSpec(memory_space=pltpu.VMEM)
        hbm = pl.BlockSpec(memory_space=pltpu.HBM)
        sums, gain, off, tsum = pl.pallas_call(
            functools.partial(head_kernel, n_dev),
            out_shape=(
                jax.ShapeDtypeStruct((groups, width, LANES), F32),
                jax.ShapeDtypeStruct((groups, n_tile, LANES), F32),
                jax.ShapeDtypeStruct((groups, n_tile, LANES), F32),
                jax.ShapeDtypeStruct((groups, LANES), F32),
            ),
            in_specs=[hbm, hbm, vmem, vmem],
            out_specs=(vmem, vmem, vmem, vmem),
            scratch_shapes=[
                pltpu.VMEM((width, depth), jnp.bfloat16),
                pltpu.VMEM((AHEAD, UNIT, DEPTH), jnp.bfloat16),
                pltpu.VMEM((UNIT, depth), jnp.bfloat16),
                pltpu.VMEM((groups, 3 * n_tile, LANES), F32),
                pltpu.VMEM((n_unit, 3, per_unit, LANES), F32),
                pltpu.VMEM((n_unit, n_dev, 3, per_unit, LANES), F32),
                pltpu.SemaphoreType.DMA((n_k,)),
                pltpu.SemaphoreType.DMA((AHEAD,)),
                pltpu.SemaphoreType.DMA((1,)),
                pltpu.SemaphoreType.DMA((n_unit, n_dev)),
                pltpu.SemaphoreType.DMA((n_unit, n_dev)),
            ],
            compiler_params=pltpu.CompilerParams(
                collective_id=0, has_side_effects=True, vmem_limit_bytes=44 * 2**20),
            name="head",
        )(h_rows, w_cols.T, tau_rows.reshape(groups, LANES), tgt_rows.reshape(groups, LANES))
        table, picked = pl.pallas_call(
            write_kernel,
            out_shape=(
                jax.ShapeDtypeStruct((width, rows), F32),
                jax.ShapeDtypeStruct((groups, LANES), F32),
            ),
            in_specs=[vmem, vmem, vmem, vmem],
            out_specs=(hbm, vmem),
            scratch_shapes=[
                pltpu.VMEM((4, TILE // 2, rows), F32),
                pltpu.SemaphoreType.DMA((4,)),
            ],
            compiler_params=pltpu.CompilerParams(vmem_limit_bytes=16 * 2**20),
            name="write",
        )(sums, gain, off, tsum)
        return table.T, picked.reshape(rows)

    return jax.shard_map(
        local_fn,
        mesh=mesh,
        in_specs=(P("dp", None), P(None, "vp"), P("dp"), P("dp")),
        out_specs=(P("dp", "vp"), P("dp")),
        check_vma=False,
    )
```

```python
import functools

import jax
import jax.numpy as jnp
from jax import lax
from jax.experimental import pallas as pl
from jax.experimental.pallas import tpu as pltpu
from jax.sharding import PartitionSpec as P

LANES = 128
SUB = 8
TILE = 80
BLOCK = 400
WIDE = 512
NARROW = 256
DEPTH = 1024
LEAD = (256, 256, 512, 512, 512)
SPREAD = 4
F32 = jnp.float32
NT = (((1,), (1,)), ((), ()))


def head_kernel(n_dev, h_hbm, w_hbm, tau_hbm, tgt_hbm, sums_ref, gain_ref, off_ref, tsum_ref,
                w_ref, h_ref, tau_ref, tgt_ref, top_ref, sum_ref, upto_ref, ltop_ref,
                snd0, snd1, rcv0, rcv1, w_sem, h_sem, in_sem, send_sem, recv_sem):
    width, depth = w_hbm.shape
    rows = h_hbm.shape[0]
    n_chunk = depth // DEPTH
    n_tile = width // TILE
    n_block = width // BLOCK
    units = [(0, WIDE), (WIDE, WIDE)]
    snd = (snd0, snd1)
    rcv = (rcv0, rcv1)
    me = lax.axis_index("vp")

    starts = []
    at = 0
    for size in LEAD:
        starts.append((at, size))
        at += size
    lead_end = at
    while at < depth:
        starts.append((at, DEPTH))
        at += DEPTH

    def copies(i, at, size):
        ks = pl.ds(at, size)
        slot = at // DEPTH
        return (pltpu.make_async_copy(h_hbm.at[pl.ds(0, WIDE), ks],
                                      h_ref.at[slot, :, pl.ds(at - slot * DEPTH, size)], h_sem.at[i]),
                pltpu.make_async_copy(w_hbm.at[:, ks], w_ref.at[:, ks], w_sem.at[i]))

    def late_copy(c):
        ks = pl.ds(pl.multiple_of(c * DEPTH, DEPTH), DEPTH)
        return pltpu.make_async_copy(h_hbm.at[pl.ds(WIDE, rows - WIDE), ks],
                                     h_ref.at[lax.rem(c + n_chunk, n_chunk + 1)], h_sem.at[len(starts) + c])

    tau_copy = pltpu.make_async_copy(tau_hbm, tau_ref, in_sem.at[0])
    tgt_copy = pltpu.make_async_copy(tgt_hbm, tgt_ref, in_sem.at[1])
    for i, (at, size) in enumerate(starts):
        for copy in copies(i, at, size):
            copy.start()
        if i == len(LEAD):
            tau_copy.start()
            tgt_copy.start()
    late_copy(0).start()

    barrier = pltpu.get_barrier_semaphore()

    @pl.loop(1, n_dev)
    def _(d):
        pl.semaphore_signal(barrier, inc=1, device_id={"vp": lax.rem(me + d, n_dev)},
                            device_id_type=pl.DeviceIdType.MESH)

    first = me * width

    def stats(t, c0, z):
        cs = slice(c0, c0 + NARROW)
        n = TILE // SUB
        z = (z * tau_ref[0:1, cs]).reshape(n, SUB, NARROW)
        top = jnp.max(jnp.max(z, axis=0), axis=0, keepdims=True)
        p = jnp.exp(z - top[None])
        token = (lax.broadcasted_iota(jnp.int32, (n, SUB, NARROW), 0) * SUB
                 + lax.broadcasted_iota(jnp.int32, (n, SUB, NARROW), 1))
        local = tgt_ref[0:1, cs] - (first + t * TILE)
        upto = jnp.sum(jnp.where(token <= local[None], p, 0.0), axis=0)
        top_ref[t:t + 1, cs] = top
        upto_ref[t:t + 1, cs] = jnp.sum(upto, axis=0, keepdims=True)
        sum_ref[t:t + 1, cs] = jnp.sum(jnp.sum(p, axis=0), axis=0, keepdims=True)
        return p

    def scan(t, c0, p):
        n = TILE // SUB
        sub = lax.broadcasted_iota(jnp.int32, (n, SUB, NARROW), 1)
        for s in (1, 2, 4):
            p = p + jnp.where(sub >= s, pltpu.roll(p, s, 1), 0.0)
        last = jnp.broadcast_to(p[:, SUB - 1:, :], (n, SUB, NARROW))
        run = last[0:1]
        parts = [p[0:1]]
        for i in range(1, n):
            parts.append(p[i:i + 1] + run)
            if i + 1 < n:
                run = run + last[i:i + 1]
        sums_ref[t * TILE:(t + 1) * TILE, c0:c0 + NARROW] = jnp.concatenate(parts, axis=0).reshape(TILE, NARROW)

    def fold(u):
        c0, wide = units[u]
        cs = slice(c0, c0 + wide)
        top = jnp.max(top_ref[:, cs], axis=0, keepdims=True)
        e = jnp.exp(top_ref[:, cs] - top)
        ltop_ref[0:1, cs] = top
        s = jnp.sum(e * sum_ref[:, cs], axis=0, keepdims=True)
        t = jnp.sum(e * upto_ref[:, cs], axis=0, keepdims=True)
        for j in range(wide // LANES):
            js = slice(j * LANES, (j + 1) * LANES)
            for i, x in enumerate((top, s, t)):
                snd[u][i, j:j + 1, :] = x[:, js]
                rcv[u][me, i, j:j + 1, :] = x[:, js]

        @pl.loop(1, n_dev)
        def _(d):
            peer = lax.rem(me + d, n_dev)
            pltpu.make_async_remote_copy(
                src_ref=snd[u], dst_ref=rcv[u].at[me], send_sem=send_sem.at[u, peer],
                recv_sem=recv_sem.at[u, me], device_id={"vp": peer},
                device_id_type=pl.DeviceIdType.MESH).start()

    def local_parts(u):
        c0, wide = units[u]
        cs = slice(c0, c0 + wide)
        e = jnp.exp(top_ref[:, cs] - ltop_ref[0:1, cs])
        gain_ref[:, cs] = e
        s = e * sum_ref[:, cs]
        run = jnp.zeros((1, wide), F32)
        for t in range(n_tile):
            off_ref[t:t + 1, cs] = run
            run = run + s[t:t + 1, :]

    def receive(u):
        c0, wide = units[u]
        per = wide // LANES
        cs = slice(c0, c0 + wide)

        @pl.loop(1, n_dev)
        def _(d):
            src = lax.rem(me + d, n_dev)
            pltpu.make_async_remote_copy(
                src_ref=snd[u], dst_ref=rcv[u].at[src], send_sem=send_sem.at[u, src],
                recv_sem=recv_sem.at[u, src], device_id={"vp": src},
                device_id_type=pl.DeviceIdType.MESH).wait()

        tops = rcv[u][:, 0]
        peak = jnp.max(tops, axis=0)
        e = jnp.exp(tops - peak[None])
        part = rcv[u][:, 1] * e
        device = lax.broadcasted_iota(jnp.int32, part.shape, 0)
        inv = 1.0 / jnp.sum(part, axis=0)
        before = jnp.sum(jnp.where(device < me, part, 0.0), axis=0) * inv
        tsum_ref[c0 // LANES:c0 // LANES + per, :] = jnp.sum(rcv[u][:, 2] * e, axis=0) * inv

        def row(x):
            return jnp.concatenate([x[j:j + 1, :] for j in range(per)], axis=1)

        f = jnp.exp(ltop_ref[0:1, cs] - row(peak)) * row(inv)
        gain_ref[:, cs] = gain_ref[:, cs] * f
        off_ref[:, cs] = off_ref[:, cs] * f + row(before)

    def add_chunk(at, size, slot, inner, init):
        for block in range(n_block):
            ws = slice(block * BLOCK, (block + 1) * BLOCK)
            z = lax.dot_general(w_ref[ws, pl.ds(at, size)], h_ref[slot, :, inner:inner + size], NT,
                                preferred_element_type=F32)
            sums_ref[ws, 0:WIDE] = z if init else sums_ref[ws, 0:WIDE] + z

    for i, (at, size) in enumerate(starts[:len(LEAD)]):
        for copy in copies(i, at, size):
            copy.wait()
        add_chunk(at, size, at // DEPTH, at % DEPTH, i == 0)
        if (at + size) % DEPTH == 0:
            late_copy((at + size) // DEPTH).start()

    lead = lead_end // DEPTH

    @pl.loop(0, (n_chunk - lead) // 2)
    def _(i):
        c = lead + 2 * i
        for b in range(2):
            for copy in copies(len(LEAD) + 2 * i + b, pl.multiple_of((c + b) * DEPTH, DEPTH), DEPTH):
                copy.wait()
        add_chunk(pl.multiple_of(c * DEPTH, DEPTH), DEPTH, c, 0, False)
        late_copy(c + 1).start()
        add_chunk(pl.multiple_of((c + 1) * DEPTH, DEPTH), DEPTH, c + 1, 0, False)

        @pl.when(c + 2 < n_chunk)
        def _():
            late_copy(c + 2).start()

    tau_copy.wait()
    tgt_copy.wait()

    zero = pl.multiple_of(me // n_dev * SUB, SUB)
    for c in range(n_chunk):
        late_copy(c).wait()
    queue = [(t, c0) for t in range(n_tile) for c0 in range(0, WIDE, NARROW)]
    per_block = BLOCK // TILE

    def block_pieces(block):
        return [(block * per_block + i, WIDE + c0) for i in range(per_block) for c0 in range(0, WIDE, NARROW)]

    def raw(t, c0):
        return sums_ref[t * TILE:(t + 1) * TILE, c0:c0 + NARROW]

    done = 0
    for block in range(n_block):
        ws = slice(block * BLOCK, (block + 1) * BLOCK)
        rs = pl.ds(block * BLOCK + zero, BLOCK)
        pieces = block_pieces(block - 1) if block else []
        reach = len(queue) * min(block + 1, SPREAD) // SPREAD
        pieces += queue[done:reach]
        done = reach
        given = 0
        for c in range(n_chunk):
            z = lax.dot_general(w_ref[ws, c * DEPTH:(c + 1) * DEPTH], h_ref[(c + n_chunk) % (n_chunk + 1)], NT,
                                preferred_element_type=F32)
            sums_ref[rs, WIDE:2 * WIDE] = z if c == 0 else sums_ref[rs, WIDE:2 * WIDE] + z
            reach = len(pieces) * (c + 1) // n_chunk
            for t, c0 in pieces[given:reach]:
                scan(t, c0, stats(t, c0, raw(t, c0)))
            given = reach
        if block == SPREAD - 1:
            pl.semaphore_wait(barrier, n_dev - 1)
            fold(0)
            local_parts(0)

    tail = block_pieces(n_block - 1)
    for t, c0 in tail:
        p = stats(t, c0, raw(t, c0))
        sums_ref[t * TILE:(t + 1) * TILE, c0:c0 + NARROW] = p.reshape(TILE, NARROW)
    fold(1)
    for t, c0 in tail:
        scan(t, c0, raw(t, c0).reshape(TILE // SUB, SUB, NARROW))
    local_parts(1)
    for v in range(2):
        receive(v)


def write_kernel(sums_ref, gain_ref, off_ref, tsum_ref, out_hbm, tgt_out, stage, sem):
    width = sums_ref.shape[0]
    n_tile = width // TILE
    tgt_out[...] = tsum_ref[...]

    def out_copy(t):
        ts = slice(t * TILE, (t + 1) * TILE)
        return pltpu.make_async_copy(stage.at[ts, :], out_hbm.at[ts, :], sem.at[t])

    for t in range(n_tile):
        ts = slice(t * TILE, (t + 1) * TILE)
        stage[ts, :] = sums_ref[ts, :] * gain_ref[t:t + 1, :] + off_ref[t:t + 1, :]
        out_copy(t).start()
    for t in range(n_tile):
        out_copy(t).wait()


def solution(mesh):
    n_dev = mesh.shape["vp"]

    def local_fn(h_rows, w_cols, tau_rows, tgt_rows):
        rows, depth = h_rows.shape
        width = w_cols.shape[1]
        groups = rows // LANES
        n_chunk = depth // DEPTH
        n_copy = len(LEAD) + (depth - sum(LEAD)) // DEPTH
        n_tile = width // TILE
        sizes = (WIDE, rows - WIDE)
        vmem = pl.BlockSpec(memory_space=pltpu.VMEM)
        hbm = pl.BlockSpec(memory_space=pltpu.HBM)
        sums, gain, off, tsum = pl.pallas_call(
            functools.partial(head_kernel, n_dev),
            out_shape=(
                jax.ShapeDtypeStruct((width, rows), F32),
                jax.ShapeDtypeStruct((n_tile, rows), F32),
                jax.ShapeDtypeStruct((n_tile, rows), F32),
                jax.ShapeDtypeStruct((groups, LANES), F32),
            ),
            in_specs=[hbm, hbm, hbm, hbm],
            out_specs=(vmem, vmem, vmem, vmem),
            scratch_shapes=[
                pltpu.VMEM((width, depth), jnp.bfloat16),
                pltpu.VMEM((n_chunk + 1, WIDE, DEPTH), jnp.bfloat16),
                pltpu.VMEM((1, rows), F32),
                pltpu.VMEM((1, rows), jnp.int32),
                pltpu.VMEM((n_tile, rows), F32),
                pltpu.VMEM((n_tile, rows), F32),
                pltpu.VMEM((n_tile, rows), F32),
                pltpu.VMEM((1, rows), F32),
                *[pltpu.VMEM((3, s // LANES, LANES), F32) for s in sizes],
                *[pltpu.VMEM((n_dev, 3, s // LANES, LANES), F32) for s in sizes],
                pltpu.SemaphoreType.DMA((n_copy,)),
                pltpu.SemaphoreType.DMA((n_copy + n_chunk,)),
                pltpu.SemaphoreType.DMA((2,)),
                pltpu.SemaphoreType.DMA((2, n_dev)),
                pltpu.SemaphoreType.DMA((2, n_dev)),
            ],
            compiler_params=pltpu.CompilerParams(
                collective_id=0, has_side_effects=True, vmem_limit_bytes=45 * 2**20),
            name="head",
        )(*[pltpu.with_memory_space_constraint(x, pltpu.HBM)
            for x in (h_rows, w_cols.T, tau_rows.reshape(1, rows), tgt_rows.reshape(1, rows))])
        table, picked = pl.pallas_call(
            write_kernel,
            out_shape=(
                jax.ShapeDtypeStruct((width, rows), F32),
                jax.ShapeDtypeStruct((groups, LANES), F32),
            ),
            in_specs=[vmem, vmem, vmem, vmem],
            out_specs=(hbm, vmem),
            scratch_shapes=[
                pltpu.VMEM((width, rows), F32),
                pltpu.SemaphoreType.DMA((n_tile,)),
            ],
            compiler_params=pltpu.CompilerParams(vmem_limit_bytes=16 * 2**20),
            name="write",
        )(sums, gain, off, tsum)
        return table.T, picked.reshape(rows)

    return jax.shard_map(
        local_fn,
        mesh=mesh,
        in_specs=(P("dp", None), P(None, "vp"), P("dp"), P("dp")),
        out_specs=(P("dp", "vp"), P("dp")),
        check_vma=False,
    )
```

```python
import functools

import jax
import jax.numpy as jnp
from jax import lax
from jax.experimental import pallas as pl
from jax.experimental.pallas import tpu as pltpu
from jax.sharding import PartitionSpec as P

LANES = 128
SUB = 8
BLOCK = 400
STRIP = 50
WIDE = 512
LOG2E = 1.4426950408889634
DEPTH = 1024
LEAD = (256, 256, 512, 512, 512)
PARTS = 5
F32 = jnp.float32
NT = (((1,), (1,)), ((), ()))


def head_kernel(n_dev, h_hbm, w_hbm, tau_hbm, tgt_hbm, sums_ref, gain_ref, off_ref, tsum_ref,
                w_ref, h_ref, tau_ref, tgt_ref, top_ref, sum_ref, upto_ref, ltop_ref,
                snd0, snd1, rcv0, rcv1, w_sem, h_sem, in_sem, send_sem, recv_sem):
    width, depth = w_hbm.shape
    rows = h_hbm.shape[0]
    n_chunk = depth // DEPTH
    per = WIDE // LANES
    n_block = width // BLOCK
    units = [(0, WIDE), (WIDE, WIDE)]
    snd = (snd0, snd1)
    rcv = (rcv0, rcv1)
    me = lax.axis_index("vp")

    starts = []
    at = 0
    for size in LEAD:
        starts.append((at, size))
        at += size
    lead_end = at
    while at < depth:
        starts.append((at, DEPTH))
        at += DEPTH

    def copies(i, at, size):
        ks = pl.ds(at, size)
        slot = at // DEPTH
        return (pltpu.make_async_copy(h_hbm.at[pl.ds(0, WIDE), ks],
                                      h_ref.at[slot, :, pl.ds(at - slot * DEPTH, size)], h_sem.at[i]),
                pltpu.make_async_copy(w_hbm.at[:, ks], w_ref.at[:, ks], w_sem.at[i]))

    def late_copy(c):
        ks = pl.ds(pl.multiple_of(c * DEPTH, DEPTH), DEPTH)
        return pltpu.make_async_copy(h_hbm.at[pl.ds(WIDE, rows - WIDE), ks],
                                     h_ref.at[lax.rem(c + n_chunk, n_chunk + 1)], h_sem.at[len(starts) + c])

    tau_copy = pltpu.make_async_copy(tau_hbm, tau_ref, in_sem.at[0])
    tgt_copy = pltpu.make_async_copy(tgt_hbm, tgt_ref, in_sem.at[1])
    for i, (at, size) in enumerate(starts):
        for copy in copies(i, at, size):
            copy.start()
        if i == len(LEAD):
            tau_copy.start()
            tgt_copy.start()
    late_copy(0).start()

    barrier = pltpu.get_barrier_semaphore()

    @pl.loop(1, n_dev)
    def _(d):
        pl.semaphore_signal(barrier, inc=1, device_id={"vp": lax.rem(me + d, n_dev)},
                            device_id_type=pl.DeviceIdType.MESH)

    first = me * width

    sub = lax.broadcasted_iota(jnp.int32, (per, SUB, LANES), 1)

    def lanes(ref, u):
        return jnp.concatenate([ref[0:1, (u * per + j) * LANES:(u * per + j + 1) * LANES][None] for j in range(per)], axis=0)

    def strip(u, block, i, value=None):
        where = (slice(u * per, (u + 1) * per), pl.ds(block * BLOCK + i, SUB, stride=STRIP), slice(None))
        if value is None:
            return sums_ref[where]
        sums_ref[where] = value

    def strips(u, block, parts):
        cuts = [STRIP * i // parts for i in range(parts + 1)]
        scale = lanes(tau_ref, u) * LOG2E
        top = None
        for lo, hi in zip(cuts, cuts[1:]):
            for i in range(lo, hi):
                z = strip(u, block, i)
                top = z if top is None else jnp.maximum(top, z)
            yield
        top = top * scale
        local = lanes(tgt_ref, u) - (first + block * BLOCK) - sub * STRIP
        run = jnp.zeros((per, SUB, LANES), F32)
        upto = run
        for lo, hi in zip(cuts, cuts[1:]):
            for i in range(lo, hi):
                run = run + jnp.exp2(strip(u, block, i) * scale - top)
                upto = jnp.where(local == i, run, upto)
                strip(u, block, i, run)
            if hi == STRIP:
                top_ref[u, block] = top
                sum_ref[u, block] = run
                upto_ref[u, block] = jnp.where(local >= STRIP, run, upto)
            yield

    def fold(u):
        top = jnp.max(jnp.max(top_ref[u], axis=0), axis=1, keepdims=True)
        e = jnp.exp2(top_ref[u] - top[None])
        ltop_ref[u] = top
        s = jnp.sum(jnp.sum(e * sum_ref[u], axis=0), axis=1, keepdims=True)
        t = jnp.sum(jnp.sum(e * upto_ref[u], axis=0), axis=1, keepdims=True)
        for j in range(per):
            for i, x in enumerate((top, s, t)):
                snd[u][i, j:j + 1, :] = x[j]
                rcv[u][me, i, j:j + 1, :] = x[j]

        @pl.loop(1, n_dev)
        def _(d):
            peer = lax.rem(me + d, n_dev)
            pltpu.make_async_remote_copy(
                src_ref=snd[u], dst_ref=rcv[u].at[me], send_sem=send_sem.at[u, peer],
                recv_sem=recv_sem.at[u, me], device_id={"vp": peer},
                device_id_type=pl.DeviceIdType.MESH).start()

    def local_parts(u):
        run = jnp.zeros((per, 1, LANES), F32)
        for block in range(n_block):
            e = jnp.exp2(top_ref[u, block] - ltop_ref[u])
            gain_ref[block, u * per:(u + 1) * per] = e
            s = e * sum_ref[u, block]
            for k in (1, 2, 4):
                s = s + jnp.where(sub >= k, pltpu.roll(s, k, 1), 0.0)
            off_ref[block, u * per:(u + 1) * per] = jnp.where(sub >= 1, pltpu.roll(s, 1, 1), 0.0) + run
            run = run + s[:, SUB - 1:, :]

    def receive(u):
        @pl.loop(1, n_dev)
        def _(d):
            src = lax.rem(me + d, n_dev)
            pltpu.make_async_remote_copy(
                src_ref=snd[u], dst_ref=rcv[u].at[src], send_sem=send_sem.at[u, src],
                recv_sem=recv_sem.at[u, src], device_id={"vp": src},
                device_id_type=pl.DeviceIdType.MESH).wait()

        tops = rcv[u][:, 0]
        peak = jnp.max(tops, axis=0)
        e = jnp.exp2(tops - peak[None])
        part = rcv[u][:, 1] * e
        device = lax.broadcasted_iota(jnp.int32, part.shape, 0)
        inv = 1.0 / jnp.sum(part, axis=0)
        before = jnp.sum(jnp.where(device < me, part, 0.0), axis=0) * inv
        tsum_ref[u * per:(u + 1) * per, :] = jnp.sum(rcv[u][:, 2] * e, axis=0) * inv

        def spread(x):
            return jnp.concatenate([x[j:j + 1, :][None] for j in range(per)], axis=0)

        f = jnp.exp2(ltop_ref[u] - spread(peak)) * spread(inv)
        before = spread(before)
        us = slice(u * per, (u + 1) * per)
        for block in range(n_block):
            gain_ref[block, us] = gain_ref[block, us] * f
            off_ref[block, us] = off_ref[block, us] * f + before

    def add(u, rs, z, init):
        for j in range(per):
            part = z[:, j * LANES:(j + 1) * LANES]
            sums_ref[u * per + j, rs, :] = part if init else sums_ref[u * per + j, rs, :] + part

    def add_chunk(at, size, slot, inner, init):
        for block in range(n_block):
            ws = slice(block * BLOCK, (block + 1) * BLOCK)
            z = lax.dot_general(w_ref[ws, pl.ds(at, size)], h_ref[slot, :, inner:inner + size], NT,
                                preferred_element_type=F32)
            add(0, ws, z, init)

    for i, (at, size) in enumerate(starts[:len(LEAD)]):
        for copy in copies(i, at, size):
            copy.wait()
        add_chunk(at, size, at // DEPTH, at % DEPTH, i == 0)
        if (at + size) % DEPTH == 0:
            late_copy((at + size) // DEPTH).start()

    lead = lead_end // DEPTH

    @pl.loop(0, (n_chunk - lead) // 2)
    def _(i):
        c = lead + 2 * i
        for b in range(2):
            for copy in copies(len(LEAD) + 2 * i + b, pl.multiple_of((c + b) * DEPTH, DEPTH), DEPTH):
                copy.wait()
        add_chunk(pl.multiple_of(c * DEPTH, DEPTH), DEPTH, c, 0, False)
        late_copy(c + 1).start()
        add_chunk(pl.multiple_of((c + 1) * DEPTH, DEPTH), DEPTH, c + 1, 0, False)

        @pl.when(c + 2 < n_chunk)
        def _():
            late_copy(c + 2).start()

    tau_copy.wait()
    tgt_copy.wait()

    zero = pl.multiple_of(me // n_dev * SUB, SUB)
    for c in range(n_chunk):
        late_copy(c).wait()
    n_step = n_chunk // 2
    first_unit = [strips(0, block, PARTS) for block in range(n_block)]
    for block in range(n_block):
        ws = slice(block * BLOCK, (block + 1) * BLOCK)
        rs = pl.ds(block * BLOCK + zero, BLOCK)
        todo = [strips(1, block - 1, PARTS)] if block else []
        for _ in range(2 if block in (0, 1) else 1 if block == 2 else 0):
            todo.append(first_unit.pop(0))
        turns = [x for x in todo for _ in range(2 * PARTS)]
        given = 0
        for c in range(n_step):
            pair = jnp.concatenate([h_ref[(2 * c + i + n_chunk) % (n_chunk + 1)] for i in range(2)], axis=1)
            z = lax.dot_general(w_ref[ws, 2 * c * DEPTH:2 * (c + 1) * DEPTH], pair, NT, preferred_element_type=F32)
            add(1, rs, z, c == 0)
            reach = len(turns) * (c + 1) // n_step
            for x in turns[given:reach]:
                next(x, None)
            given = reach
        if block == 2:
            pl.semaphore_wait(barrier, n_dev - 1)
            fold(0)
            local_parts(0)

    for _ in strips(1, n_block - 1, 1):
        pass
    fold(1)
    local_parts(1)
    for v in range(2):
        receive(v)


def write_kernel(sums_ref, gain_ref, off_ref, tsum_ref, out_hbm, tgt_out, stage, sem):
    groups, width, _ = sums_ref.shape
    n_block = width // BLOCK
    tgt_out[...] = tsum_ref[...]

    def out_copy(block, g):
        rs = slice(block * BLOCK, (block + 1) * BLOCK)
        return pltpu.make_async_copy(stage.at[g, rs, :], out_hbm.at[rs, g * LANES:(g + 1) * LANES], sem.at[block, g])

    for block in range(n_block):
        for g in range(groups):
            gain = gain_ref[block, g]
            off = off_ref[block, g]
            for i in range(STRIP):
                rows = pl.ds(block * BLOCK + i, SUB, stride=STRIP)
                stage[g, rows, :] = sums_ref[g, rows, :] * gain + off
            out_copy(block, g).start()
    for block in range(n_block):
        for g in range(groups):
            out_copy(block, g).wait()


def solution(mesh):
    n_dev = mesh.shape["vp"]

    def local_fn(h_rows, w_cols, tau_rows, tgt_rows):
        rows, depth = h_rows.shape
        width = w_cols.shape[1]
        groups = rows // LANES
        n_chunk = depth // DEPTH
        n_copy = len(LEAD) + (depth - sum(LEAD)) // DEPTH
        n_block = width // BLOCK
        per = WIDE // LANES
        n_unit = rows // WIDE
        vmem = pl.BlockSpec(memory_space=pltpu.VMEM)
        hbm = pl.BlockSpec(memory_space=pltpu.HBM)
        sums, gain, off, tsum = pl.pallas_call(
            functools.partial(head_kernel, n_dev),
            out_shape=(
                jax.ShapeDtypeStruct((groups, width, LANES), F32),
                jax.ShapeDtypeStruct((n_block, groups, SUB, LANES), F32),
                jax.ShapeDtypeStruct((n_block, groups, SUB, LANES), F32),
                jax.ShapeDtypeStruct((groups, LANES), F32),
            ),
            in_specs=[hbm, hbm, hbm, hbm],
            out_specs=(vmem, vmem, vmem, vmem),
            scratch_shapes=[
                pltpu.VMEM((width, depth), jnp.bfloat16),
                pltpu.VMEM((n_chunk + 1, WIDE, DEPTH), jnp.bfloat16),
                pltpu.VMEM((1, rows), F32),
                pltpu.VMEM((1, rows), jnp.int32),
                *[pltpu.VMEM((n_unit, n_block, per, SUB, LANES), F32) for _ in range(3)],
                pltpu.VMEM((n_unit, per, 1, LANES), F32),
                *[pltpu.VMEM((3, per, LANES), F32) for _ in range(n_unit)],
                *[pltpu.VMEM((n_dev, 3, per, LANES), F32) for _ in range(n_unit)],
                pltpu.SemaphoreType.DMA((n_copy,)),
                pltpu.SemaphoreType.DMA((n_copy + n_chunk,)),
                pltpu.SemaphoreType.DMA((2,)),
                pltpu.SemaphoreType.DMA((2, n_dev)),
                pltpu.SemaphoreType.DMA((2, n_dev)),
            ],
            compiler_params=pltpu.CompilerParams(
                collective_id=0, has_side_effects=True, vmem_limit_bytes=45 * 2**20),
            name="head",
        )(*[pltpu.with_memory_space_constraint(x, pltpu.HBM)
            for x in (h_rows, w_cols.T, tau_rows.reshape(1, rows), tgt_rows.reshape(1, rows))])
        table, picked = pl.pallas_call(
            write_kernel,
            out_shape=(
                jax.ShapeDtypeStruct((width, rows), F32),
                jax.ShapeDtypeStruct((groups, LANES), F32),
            ),
            in_specs=[vmem, vmem, vmem, vmem],
            out_specs=(hbm, vmem),
            scratch_shapes=[
                pltpu.VMEM((groups, width, LANES), F32),
                pltpu.SemaphoreType.DMA((n_block, groups)),
            ],
            compiler_params=pltpu.CompilerParams(vmem_limit_bytes=16 * 2**20),
            name="write",
        )(sums, gain, off, tsum)
        return table.T, picked.reshape(rows)

    return jax.shard_map(
        local_fn,
        mesh=mesh,
        in_specs=(P("dp", None), P(None, "vp"), P("dp"), P("dp")),
        out_specs=(P("dp", "vp"), P("dp")),
        check_vma=False,
    )
```

```python
import functools

import jax
import jax.numpy as jnp
from jax import lax
from jax.experimental import pallas as pl
from jax.experimental.pallas import tpu as pltpu
from jax.sharding import PartitionSpec as P

LANES = 128
SUB = 8
BLOCK = 400
STRIP = 50
WIDE = 512
LOG2E = 1.4426950408889634
DEPTH = 1024
LEAD = (256, 256, 512, 512, 512)
PARTS = 5
F32 = jnp.float32
NT = (((1,), (1,)), ((), ()))


def head_kernel(n_dev, h_hbm, w_hbm, tau_hbm, tgt_hbm, sums_ref, gain_ref, off_ref, tsum_ref,
                w_ref, h_ref, tau_ref, tgt_ref, top_ref, sum_ref, upto_ref, ltop_ref,
                snd0, snd1, rcv0, rcv1, w_sem, h_sem, in_sem, send_sem, recv_sem):
    width, depth = w_hbm.shape
    rows = h_hbm.shape[0]
    n_chunk = depth // DEPTH
    per = WIDE // LANES
    n_block = width // BLOCK
    units = [(0, WIDE), (WIDE, WIDE)]
    snd = (snd0, snd1)
    rcv = (rcv0, rcv1)
    me = lax.axis_index("vp")

    starts = []
    at = 0
    for size in LEAD:
        starts.append((at, size))
        at += size
    lead_end = at
    while at < depth:
        starts.append((at, DEPTH))
        at += DEPTH

    def copies(i, at, size):
        ks = pl.ds(at, size)
        slot = at // DEPTH
        return (pltpu.make_async_copy(h_hbm.at[pl.ds(0, WIDE), ks],
                                      h_ref.at[slot, :, pl.ds(at - slot * DEPTH, size)], h_sem.at[i]),
                pltpu.make_async_copy(w_hbm.at[:, ks], w_ref.at[:, ks], w_sem.at[i]))

    def late_copy(c):
        ks = pl.ds(pl.multiple_of(c * DEPTH, DEPTH), DEPTH)
        return pltpu.make_async_copy(h_hbm.at[pl.ds(WIDE, rows - WIDE), ks],
                                     h_ref.at[lax.rem(c + n_chunk, n_chunk + 1)], h_sem.at[len(starts) + c])

    tau_copy = pltpu.make_async_copy(tau_hbm, tau_ref, in_sem.at[0])
    tgt_copy = pltpu.make_async_copy(tgt_hbm, tgt_ref, in_sem.at[1])
    for i, (at, size) in enumerate(starts):
        for copy in copies(i, at, size):
            copy.start()
        if i == len(LEAD):
            tau_copy.start()
            tgt_copy.start()
    late_copy(0).start()

    barrier = pltpu.get_barrier_semaphore()

    @pl.loop(1, n_dev)
    def _(d):
        pl.semaphore_signal(barrier, inc=1, device_id={"vp": lax.rem(me + d, n_dev)},
                            device_id_type=pl.DeviceIdType.MESH)

    first = me * width

    sub = lax.broadcasted_iota(jnp.int32, (per, SUB, LANES), 1)

    def lanes(ref, u):
        return jnp.concatenate([ref[0:1, (u * per + j) * LANES:(u * per + j + 1) * LANES][None] for j in range(per)], axis=0)

    def strip(u, block, i, value=None):
        where = (slice(u * per, (u + 1) * per), pl.ds(block * BLOCK + i, SUB, stride=STRIP), slice(None))
        if value is None:
            return sums_ref[where]
        sums_ref[where] = value

    def strips(u, block, parts):
        cuts = [STRIP * i // parts for i in range(parts + 1)]
        scale = lanes(tau_ref, u) * LOG2E
        top = None
        for lo, hi in zip(cuts, cuts[1:]):
            for i in range(lo, hi):
                z = strip(u, block, i)
                top = z if top is None else jnp.maximum(top, z)
            yield
        top = top * scale
        local = lanes(tgt_ref, u) - (first + block * BLOCK) - sub * STRIP
        run = jnp.zeros((per, SUB, LANES), F32)
        upto = run
        for lo, hi in zip(cuts, cuts[1:]):
            for i in range(lo, hi):
                run = run + jnp.exp2(strip(u, block, i) * scale - top)
                upto = jnp.where(local == i, run, upto)
                strip(u, block, i, run)
            if hi == STRIP:
                top_ref[u, block] = top
                sum_ref[u, block] = run
                upto_ref[u, block] = jnp.where(local >= STRIP, run, upto)
            yield

    def fold(u):
        top = jnp.max(jnp.max(top_ref[u], axis=0), axis=1, keepdims=True)
        e = jnp.exp2(top_ref[u] - top[None])
        ltop_ref[u] = top
        s = jnp.sum(jnp.sum(e * sum_ref[u], axis=0), axis=1, keepdims=True)
        t = jnp.sum(jnp.sum(e * upto_ref[u], axis=0), axis=1, keepdims=True)
        for j in range(per):
            for i, x in enumerate((top, s, t)):
                snd[u][i, j:j + 1, :] = x[j]
                rcv[u][me, i, j:j + 1, :] = x[j]

        @pl.loop(1, n_dev)
        def _(d):
            peer = lax.rem(me + d, n_dev)
            pltpu.make_async_remote_copy(
                src_ref=snd[u], dst_ref=rcv[u].at[me], send_sem=send_sem.at[u, peer],
                recv_sem=recv_sem.at[u, me], device_id={"vp": peer},
                device_id_type=pl.DeviceIdType.MESH).start()

    def local_parts(u):
        run = jnp.zeros((per, 1, LANES), F32)
        for block in range(n_block):
            e = jnp.exp2(top_ref[u, block] - ltop_ref[u])
            gain_ref[block, u * per:(u + 1) * per] = e
            s = e * sum_ref[u, block]
            for k in (1, 2, 4):
                s = s + jnp.where(sub >= k, pltpu.roll(s, k, 1), 0.0)
            off_ref[block, u * per:(u + 1) * per] = jnp.where(sub >= 1, pltpu.roll(s, 1, 1), 0.0) + run
            run = run + s[:, SUB - 1:, :]

    def receive(u):
        @pl.loop(1, n_dev)
        def _(d):
            src = lax.rem(me + d, n_dev)
            pltpu.make_async_remote_copy(
                src_ref=snd[u], dst_ref=rcv[u].at[src], send_sem=send_sem.at[u, src],
                recv_sem=recv_sem.at[u, src], device_id={"vp": src},
                device_id_type=pl.DeviceIdType.MESH).wait()

        tops = rcv[u][:, 0]
        peak = jnp.max(tops, axis=0)
        e = jnp.exp2(tops - peak[None])
        part = rcv[u][:, 1] * e
        device = lax.broadcasted_iota(jnp.int32, part.shape, 0)
        inv = 1.0 / jnp.sum(part, axis=0)
        before = jnp.sum(jnp.where(device < me, part, 0.0), axis=0) * inv
        tsum_ref[u * per:(u + 1) * per, :] = jnp.sum(rcv[u][:, 2] * e, axis=0) * inv

        def spread(x):
            return jnp.concatenate([x[j:j + 1, :][None] for j in range(per)], axis=0)

        f = jnp.exp2(ltop_ref[u] - spread(peak)) * spread(inv)
        before = spread(before)
        us = slice(u * per, (u + 1) * per)
        for block in range(n_block):
            gain_ref[block, us] = gain_ref[block, us] * f
            off_ref[block, us] = off_ref[block, us] * f + before

    def add(u, rs, z, init):
        for j in range(per):
            part = z[:, j * LANES:(j + 1) * LANES]
            sums_ref[u * per + j, rs, :] = part if init else sums_ref[u * per + j, rs, :] + part

    def add_chunk(at, size, slot, inner, init):
        for block in range(n_block):
            ws = slice(block * BLOCK, (block + 1) * BLOCK)
            z = lax.dot_general(w_ref[ws, pl.ds(at, size)], h_ref[slot, :, inner:inner + size], NT,
                                preferred_element_type=F32)
            add(0, ws, z, init)

    for i, (at, size) in enumerate(starts[:len(LEAD)]):
        for copy in copies(i, at, size):
            copy.wait()
        add_chunk(at, size, at // DEPTH, at % DEPTH, i == 0)
        if (at + size) % DEPTH == 0:
            late_copy((at + size) // DEPTH).start()

    lead = lead_end // DEPTH

    @pl.loop(0, (n_chunk - lead) // 2)
    def _(i):
        c = lead + 2 * i
        for b in range(2):
            for copy in copies(len(LEAD) + 2 * i + b, pl.multiple_of((c + b) * DEPTH, DEPTH), DEPTH):
                copy.wait()
        add_chunk(pl.multiple_of(c * DEPTH, DEPTH), DEPTH, c, 0, False)
        late_copy(c + 1).start()
        add_chunk(pl.multiple_of((c + 1) * DEPTH, DEPTH), DEPTH, c + 1, 0, False)

        @pl.when(c + 2 < n_chunk)
        def _():
            late_copy(c + 2).start()

    tau_copy.wait()
    tgt_copy.wait()

    zero = pl.multiple_of(me // n_dev * SUB, SUB)
    for c in range(n_chunk):
        late_copy(c).wait()
    n_step = n_chunk // 2
    first_unit = [strips(0, block, PARTS) for block in range(n_block)]
    for block in range(n_block):
        ws = slice(block * BLOCK, (block + 1) * BLOCK)
        rs = pl.ds(block * BLOCK + zero, BLOCK)
        todo = [strips(1, block - 1, PARTS)] if block else []
        for _ in range(2 if block in (0, 1) else 1 if block == 2 else 0):
            todo.append(first_unit.pop(0))
        turns = [x for x in todo for _ in range(2 * PARTS)]
        given = 0
        for c in range(n_step):
            pair = jnp.concatenate([h_ref[(2 * c + i + n_chunk) % (n_chunk + 1)] for i in range(2)], axis=1)
            z = lax.dot_general(w_ref[ws, 2 * c * DEPTH:2 * (c + 1) * DEPTH], pair, NT, preferred_element_type=F32)
            add(1, rs, z, c == 0)
            reach = len(turns) * (c + 1) // n_step
            for x in turns[given:reach]:
                next(x, None)
            given = reach
        if block == 2:
            pl.semaphore_wait(barrier, n_dev - 1)
            fold(0)

    for _ in strips(1, n_block - 1, 1):
        pass
    fold(1)
    local_parts(0)
    receive(0)
    local_parts(1)
    for block in range(n_block):
        gain = gain_ref[block, 0:per]
        off = off_ref[block, 0:per]
        for i in range(STRIP):
            strip(0, block, i, strip(0, block, i) * gain + off)
    receive(1)


def write_kernel(sums_ref, gain_ref, off_ref, tsum_ref, out_hbm, tgt_out, stage, sem):
    groups, width, _ = sums_ref.shape
    n_block = width // BLOCK
    tgt_out[...] = tsum_ref[...]

    def out_copy(block, g, source, at=None):
        rs = slice(block * BLOCK, (block + 1) * BLOCK)
        return pltpu.make_async_copy(source.at[g if at is None else at, rs, :], out_hbm.at[rs, g * LANES:(g + 1) * LANES], sem.at[block, g])

    ready = WIDE // LANES
    for block in range(n_block):
        for g in range(ready):
            out_copy(block, g, sums_ref).start()
    for block in range(n_block):
        for g in range(ready, groups):
            gain = gain_ref[block, g]
            off = off_ref[block, g]
            for i in range(STRIP):
                rows = pl.ds(block * BLOCK + i, SUB, stride=STRIP)
                stage[g - ready, rows, :] = sums_ref[g, rows, :] * gain + off
            out_copy(block, g, stage, g - ready).start()
    for block in range(n_block):
        for g in range(groups):
            if g < ready:
                out_copy(block, g, sums_ref).wait()
            else:
                out_copy(block, g, stage, g - ready).wait()


def solution(mesh):
    n_dev = mesh.shape["vp"]

    def local_fn(h_rows, w_cols, tau_rows, tgt_rows):
        rows, depth = h_rows.shape
        width = w_cols.shape[1]
        groups = rows // LANES
        n_chunk = depth // DEPTH
        n_copy = len(LEAD) + (depth - sum(LEAD)) // DEPTH
        n_block = width // BLOCK
        per = WIDE // LANES
        n_unit = rows // WIDE
        vmem = pl.BlockSpec(memory_space=pltpu.VMEM)
        hbm = pl.BlockSpec(memory_space=pltpu.HBM)
        sums, gain, off, tsum = pl.pallas_call(
            functools.partial(head_kernel, n_dev),
            out_shape=(
                jax.ShapeDtypeStruct((groups, width, LANES), F32),
                jax.ShapeDtypeStruct((n_block, groups, SUB, LANES), F32),
                jax.ShapeDtypeStruct((n_block, groups, SUB, LANES), F32),
                jax.ShapeDtypeStruct((groups, LANES), F32),
            ),
            in_specs=[hbm, hbm, hbm, hbm],
            out_specs=(vmem, vmem, vmem, vmem),
            scratch_shapes=[
                pltpu.VMEM((width, depth), jnp.bfloat16),
                pltpu.VMEM((n_chunk + 1, WIDE, DEPTH), jnp.bfloat16),
                pltpu.VMEM((1, rows), F32),
                pltpu.VMEM((1, rows), jnp.int32),
                *[pltpu.VMEM((n_unit, n_block, per, SUB, LANES), F32) for _ in range(3)],
                pltpu.VMEM((n_unit, per, 1, LANES), F32),
                *[pltpu.VMEM((3, per, LANES), F32) for _ in range(n_unit)],
                *[pltpu.VMEM((n_dev, 3, per, LANES), F32) for _ in range(n_unit)],
                pltpu.SemaphoreType.DMA((n_copy,)),
                pltpu.SemaphoreType.DMA((n_copy + n_chunk,)),
                pltpu.SemaphoreType.DMA((2,)),
                pltpu.SemaphoreType.DMA((2, n_dev)),
                pltpu.SemaphoreType.DMA((2, n_dev)),
            ],
            compiler_params=pltpu.CompilerParams(
                collective_id=0, has_side_effects=True, vmem_limit_bytes=45 * 2**20),
            name="head",
        )(*[pltpu.with_memory_space_constraint(x, pltpu.HBM)
            for x in (h_rows, w_cols.T, tau_rows.reshape(1, rows), tgt_rows.reshape(1, rows))])
        table, picked = pl.pallas_call(
            write_kernel,
            out_shape=(
                jax.ShapeDtypeStruct((width, rows), F32),
                jax.ShapeDtypeStruct((groups, LANES), F32),
            ),
            in_specs=[vmem, vmem, vmem, vmem],
            out_specs=(hbm, vmem),
            scratch_shapes=[
                pltpu.VMEM((groups - per, width, LANES), F32),
                pltpu.SemaphoreType.DMA((n_block, groups)),
            ],
            compiler_params=pltpu.CompilerParams(vmem_limit_bytes=16 * 2**20),
            name="write",
        )(sums, gain, off, tsum)
        return table.T, picked.reshape(rows)

    return jax.shard_map(
        local_fn,
        mesh=mesh,
        in_specs=(P("dp", None), P(None, "vp"), P("dp"), P("dp")),
        out_specs=(P("dp", "vp"), P("dp")),
        check_vma=False,
    )
```

```python
import functools

import jax
import jax.numpy as jnp
from jax import lax
from jax.experimental import pallas as pl
from jax.experimental.pallas import tpu as pltpu
from jax.sharding import PartitionSpec as P

LANES = 128
SUB = 8
BLOCK = 400
STRIP = 50
WIDE = 512
LOG2E = 1.4426950408889634
DEPTH = 1024
LEAD = (256, 256, 512, 512, 512)
PARTS = 5
F32 = jnp.float32
NT = (((1,), (1,)), ((), ()))


def head_kernel(n_dev, h_hbm, w_hbm, tau_hbm, tgt_hbm, sums_ref, gain_ref, off_ref, tsum_ref,
                w_ref, h_ref, tau_ref, tgt_ref, top_ref, sum_ref, upto_ref, ltop_ref,
                snd0, snd1, rcv0, rcv1, w_sem, h_sem, in_sem, send_sem, recv_sem):
    width, depth = w_hbm.shape
    rows = h_hbm.shape[0]
    n_chunk = depth // DEPTH
    per = WIDE // LANES
    n_block = width // BLOCK
    units = [(0, WIDE), (WIDE, WIDE)]
    snd = (snd0, snd1)
    rcv = (rcv0, rcv1)
    me = lax.axis_index("vp")

    starts = []
    at = 0
    for size in LEAD:
        starts.append((at, size))
        at += size
    lead_end = at
    while at < depth:
        starts.append((at, DEPTH))
        at += DEPTH

    def copies(i, at, size):
        ks = pl.ds(at, size)
        slot = at // DEPTH
        return (pltpu.make_async_copy(h_hbm.at[pl.ds(0, WIDE), ks],
                                      h_ref.at[slot, :, pl.ds(at - slot * DEPTH, size)], h_sem.at[i]),
                pltpu.make_async_copy(w_hbm.at[:, ks], w_ref.at[:, ks], w_sem.at[i]))

    def late_copy(c):
        ks = pl.ds(pl.multiple_of(c * DEPTH, DEPTH), DEPTH)
        return pltpu.make_async_copy(h_hbm.at[pl.ds(WIDE, rows - WIDE), ks],
                                     h_ref.at[lax.rem(c + n_chunk, n_chunk + 1)], h_sem.at[len(starts) + c])

    tau_copy = pltpu.make_async_copy(tau_hbm, tau_ref, in_sem.at[0])
    tgt_copy = pltpu.make_async_copy(tgt_hbm, tgt_ref, in_sem.at[1])
    for i, (at, size) in enumerate(starts):
        for copy in copies(i, at, size):
            copy.start()
        if i == len(LEAD):
            tau_copy.start()
            tgt_copy.start()
    late_copy(0).start()

    barrier = pltpu.get_barrier_semaphore()

    @pl.loop(1, n_dev)
    def _(d):
        pl.semaphore_signal(barrier, inc=1, device_id={"vp": lax.rem(me + d, n_dev)},
                            device_id_type=pl.DeviceIdType.MESH)

    first = me * width

    sub = lax.broadcasted_iota(jnp.int32, (per, SUB, LANES), 1)

    def lanes(ref, u):
        return jnp.concatenate([ref[0:1, (u * per + j) * LANES:(u * per + j + 1) * LANES][None] for j in range(per)], axis=0)

    def strip(u, block, i, value=None):
        where = (slice(u * per, (u + 1) * per), pl.ds(block * BLOCK + i, SUB, stride=STRIP), slice(None))
        if value is None:
            return sums_ref[where]
        sums_ref[where] = value

    def strips(u, block, parts):
        cuts = [STRIP * i // parts for i in range(parts + 1)]
        scale = lanes(tau_ref, u) * LOG2E
        top = None
        for lo, hi in zip(cuts, cuts[1:]):
            for i in range(lo, hi):
                z = strip(u, block, i)
                top = z if top is None else jnp.maximum(top, z)
            yield
        top = top * scale
        local = lanes(tgt_ref, u) - (first + block * BLOCK) - sub * STRIP
        run = jnp.zeros((per, SUB, LANES), F32)
        upto = run
        for lo, hi in zip(cuts, cuts[1:]):
            for i in range(lo, hi):
                run = run + jnp.exp2(strip(u, block, i) * scale - top)
                upto = jnp.where(local == i, run, upto)
                strip(u, block, i, run)
            if hi == STRIP:
                top_ref[u, block] = top
                sum_ref[u, block] = run
                upto_ref[u, block] = jnp.where(local >= STRIP, run, upto)
            yield

    def fold(u):
        top = jnp.max(jnp.max(top_ref[u], axis=0), axis=1, keepdims=True)
        e = jnp.exp2(top_ref[u] - top[None])
        ltop_ref[u] = top
        s = jnp.sum(jnp.sum(e * sum_ref[u], axis=0), axis=1, keepdims=True)
        t = jnp.sum(jnp.sum(e * upto_ref[u], axis=0), axis=1, keepdims=True)
        for j in range(per):
            for i, x in enumerate((top, s, t)):
                snd[u][i, j:j + 1, :] = x[j]
                rcv[u][me, i, j:j + 1, :] = x[j]

        @pl.loop(1, n_dev)
        def _(d):
            peer = lax.rem(me + d, n_dev)
            pltpu.make_async_remote_copy(
                src_ref=snd[u], dst_ref=rcv[u].at[me], send_sem=send_sem.at[u, peer],
                recv_sem=recv_sem.at[u, me], device_id={"vp": peer},
                device_id_type=pl.DeviceIdType.MESH).start()

    def local_parts(u):
        run = jnp.zeros((per, 1, LANES), F32)
        for block in range(n_block):
            e = jnp.exp2(top_ref[u, block] - ltop_ref[u])
            gain_ref[block, u * per:(u + 1) * per] = e
            s = e * sum_ref[u, block]
            for k in (1, 2, 4):
                s = s + jnp.where(sub >= k, pltpu.roll(s, k, 1), 0.0)
            off_ref[block, u * per:(u + 1) * per] = jnp.where(sub >= 1, pltpu.roll(s, 1, 1), 0.0) + run
            run = run + s[:, SUB - 1:, :]

    def receive(u):
        @pl.loop(1, n_dev)
        def _(d):
            src = lax.rem(me + d, n_dev)
            pltpu.make_async_remote_copy(
                src_ref=snd[u], dst_ref=rcv[u].at[src], send_sem=send_sem.at[u, src],
                recv_sem=recv_sem.at[u, src], device_id={"vp": src},
                device_id_type=pl.DeviceIdType.MESH).wait()

        tops = rcv[u][:, 0]
        peak = jnp.max(tops, axis=0)
        e = jnp.exp2(tops - peak[None])
        part = rcv[u][:, 1] * e
        device = lax.broadcasted_iota(jnp.int32, part.shape, 0)
        inv = 1.0 / jnp.sum(part, axis=0)
        before = jnp.sum(jnp.where(device < me, part, 0.0), axis=0) * inv
        tsum_ref[u * per:(u + 1) * per, :] = jnp.sum(rcv[u][:, 2] * e, axis=0) * inv

        def spread(x):
            return jnp.concatenate([x[j:j + 1, :][None] for j in range(per)], axis=0)

        f = jnp.exp2(ltop_ref[u] - spread(peak)) * spread(inv)
        before = spread(before)
        us = slice(u * per, (u + 1) * per)
        for block in range(n_block):
            gain_ref[block, us] = gain_ref[block, us] * f
            off_ref[block, us] = off_ref[block, us] * f + before

    def add(u, rs, z, init):
        for j in range(per):
            part = z[:, j * LANES:(j + 1) * LANES]
            sums_ref[u * per + j, rs, :] = part if init else sums_ref[u * per + j, rs, :] + part

    def add_chunk(at, size, slot, inner, init):
        for block in range(n_block):
            ws = slice(block * BLOCK, (block + 1) * BLOCK)
            z = lax.dot_general(w_ref[ws, pl.ds(at, size)], h_ref[slot, :, inner:inner + size], NT,
                                preferred_element_type=F32)
            add(0, ws, z, init)

    for i, (at, size) in enumerate(starts[:len(LEAD)]):
        for copy in copies(i, at, size):
            copy.wait()
        add_chunk(at, size, at // DEPTH, at % DEPTH, i == 0)
        if (at + size) % DEPTH == 0:
            late_copy((at + size) // DEPTH).start()

    lead = lead_end // DEPTH

    @pl.loop(0, (n_chunk - lead) // 2)
    def _(i):
        c = lead + 2 * i
        for b in range(2):
            for copy in copies(len(LEAD) + 2 * i + b, pl.multiple_of((c + b) * DEPTH, DEPTH), DEPTH):
                copy.wait()
        add_chunk(pl.multiple_of(c * DEPTH, DEPTH), DEPTH, c, 0, False)
        late_copy(c + 1).start()
        add_chunk(pl.multiple_of((c + 1) * DEPTH, DEPTH), DEPTH, c + 1, 0, False)

        @pl.when(c + 2 < n_chunk)
        def _():
            late_copy(c + 2).start()

    tau_copy.wait()
    tgt_copy.wait()

    zero = pl.multiple_of(me // n_dev * SUB, SUB)
    for c in range(n_chunk):
        late_copy(c).wait()
    n_step = n_chunk // 2
    first_unit = [strips(0, block, PARTS) for block in range(n_block)]
    for block in range(n_block):
        ws = slice(block * BLOCK, (block + 1) * BLOCK)
        rs = pl.ds(block * BLOCK + zero, BLOCK)
        todo = [strips(1, block - 1, PARTS)] if block else []
        for _ in range(2 if block in (0, 1) else 1 if block == 2 else 0):
            todo.append(first_unit.pop(0))
        turns = [x for x in todo for _ in range(2 * PARTS)]
        given = 0
        for c in range(n_step):
            pair = jnp.concatenate([h_ref[(2 * c + i + n_chunk) % (n_chunk + 1)] for i in range(2)], axis=1)
            z = lax.dot_general(w_ref[ws, 2 * c * DEPTH:2 * (c + 1) * DEPTH], pair, NT, preferred_element_type=F32)
            add(1, rs, z, c == 0)
            reach = len(turns) * (c + 1) // n_step
            for x in turns[given:reach]:
                next(x, None)
            given = reach
        if block == 2:
            pl.semaphore_wait(barrier, n_dev - 1)
            fold(0)

    for _ in strips(1, n_block - 1, 1):
        pass
    fold(1)
    local_parts(0)
    receive(0)
    local_parts(1)
    for block in range(n_block):
        gain = gain_ref[block, 0:per]
        off = off_ref[block, 0:per]
        for i in range(STRIP):
            strip(0, block, i, strip(0, block, i) * gain + off)
    receive(1)


def write_kernel(sums_ref, gain_ref, off_ref, tsum_ref, out_hbm, tgt_out, stage, sem):
    groups, width, _ = sums_ref.shape
    n_block = width // BLOCK
    tgt_out[...] = tsum_ref[...]

    def out_copy(block, g, source, at=None):
        rs = slice(block * BLOCK, (block + 1) * BLOCK)
        return pltpu.make_async_copy(source.at[g if at is None else at, rs, :], out_hbm.at[rs, g * LANES:(g + 1) * LANES], sem.at[block, g])

    ready = WIDE // LANES
    for block in range(n_block):
        for g in range(ready):
            out_copy(block, g, sums_ref).start(priority=g % 2)
    for block in range(n_block):
        for g in range(ready, groups):
            gain = gain_ref[block, g]
            off = off_ref[block, g]
            for i in range(STRIP):
                rows = pl.ds(block * BLOCK + i, SUB, stride=STRIP)
                stage[g - ready, rows, :] = sums_ref[g, rows, :] * gain + off
            out_copy(block, g, stage, g - ready).start(priority=g % 2)
    for block in range(n_block):
        for g in range(groups):
            if g < ready:
                out_copy(block, g, sums_ref).wait()
            else:
                out_copy(block, g, stage, g - ready).wait()


def solution(mesh):
    n_dev = mesh.shape["vp"]

    def local_fn(h_rows, w_cols, tau_rows, tgt_rows):
        rows, depth = h_rows.shape
        width = w_cols.shape[1]
        groups = rows // LANES
        n_chunk = depth // DEPTH
        n_copy = len(LEAD) + (depth - sum(LEAD)) // DEPTH
        n_block = width // BLOCK
        per = WIDE // LANES
        n_unit = rows // WIDE
        vmem = pl.BlockSpec(memory_space=pltpu.VMEM)
        hbm = pl.BlockSpec(memory_space=pltpu.HBM)
        sums, gain, off, tsum = pl.pallas_call(
            functools.partial(head_kernel, n_dev),
            out_shape=(
                jax.ShapeDtypeStruct((groups, width, LANES), F32),
                jax.ShapeDtypeStruct((n_block, groups, SUB, LANES), F32),
                jax.ShapeDtypeStruct((n_block, groups, SUB, LANES), F32),
                jax.ShapeDtypeStruct((groups, LANES), F32),
            ),
            in_specs=[hbm, hbm, hbm, hbm],
            out_specs=(vmem, vmem, vmem, vmem),
            scratch_shapes=[
                pltpu.VMEM((width, depth), jnp.bfloat16),
                pltpu.VMEM((n_chunk + 1, WIDE, DEPTH), jnp.bfloat16),
                pltpu.VMEM((1, rows), F32),
                pltpu.VMEM((1, rows), jnp.int32),
                *[pltpu.VMEM((n_unit, n_block, per, SUB, LANES), F32) for _ in range(3)],
                pltpu.VMEM((n_unit, per, 1, LANES), F32),
                *[pltpu.VMEM((3, per, LANES), F32) for _ in range(n_unit)],
                *[pltpu.VMEM((n_dev, 3, per, LANES), F32) for _ in range(n_unit)],
                pltpu.SemaphoreType.DMA((n_copy,)),
                pltpu.SemaphoreType.DMA((n_copy + n_chunk,)),
                pltpu.SemaphoreType.DMA((2,)),
                pltpu.SemaphoreType.DMA((2, n_dev)),
                pltpu.SemaphoreType.DMA((2, n_dev)),
            ],
            compiler_params=pltpu.CompilerParams(
                collective_id=0, has_side_effects=True, vmem_limit_bytes=45 * 2**20),
            name="head",
        )(*[pltpu.with_memory_space_constraint(x, pltpu.HBM)
            for x in (h_rows, w_cols.T, tau_rows.reshape(1, rows), tgt_rows.reshape(1, rows))])
        table, picked = pl.pallas_call(
            write_kernel,
            out_shape=(
                jax.ShapeDtypeStruct((width, rows), F32),
                jax.ShapeDtypeStruct((groups, LANES), F32),
            ),
            in_specs=[vmem, vmem, vmem, vmem],
            out_specs=(hbm, vmem),
            scratch_shapes=[
                pltpu.VMEM((groups - per, width, LANES), F32),
                pltpu.SemaphoreType.DMA((n_block, groups)),
            ],
            compiler_params=pltpu.CompilerParams(vmem_limit_bytes=16 * 2**20),
            name="write",
        )(sums, gain, off, tsum)
        return table.T, picked.reshape(rows)

    return jax.shard_map(
        local_fn,
        mesh=mesh,
        in_specs=(P("dp", None), P(None, "vp"), P("dp"), P("dp")),
        out_specs=(P("dp", "vp"), P("dp")),
        check_vma=False,
    )
```
